32 devices in a mesh: dp: 4 (over y, core), tp: 8 (over z, x).
Axes of the slice: x: 2, y: 2, z: 4, core: 2. Of those that a mesh axis runs over, the one named last changes fastest.
Arguments:
- gate_master: float32 [8192, 16384], P(('dp', 'tp')), may hold values from -0.0625 to 0.0625
- up_master: float32 [8192, 16384], P(('dp', 'tp')), may hold values from -0.0625 to 0.0625
- down_master: float32 [16384, 8192], P(None, ('dp', 'tp')), may hold values from -0.046875 to 0.046875
- out_proj: bfloat16 [8192, 8192], P(None, 'tp'), may hold values from -0.0625 to 0.0625
- norm_gain: float32 [8192], replicated, may hold values from 0.1 to 1.9
- residual_in: bfloat16 [256, 8192], P('dp', 'tp'), may hold values from -6 to 6
- queries: bfloat16 [256, 64, 128], P(('dp', 'tp')), may hold values from -150 to 150
- new_keys: bfloat16 [256, 8, 128], P(('dp', 'tp')), may hold values from -5 to 5
- new_values: bfloat16 [256, 8, 128], P(('dp', 'tp')), may hold values from -5 to 5
- cache_keys: bfloat16 [256, 256, 8, 128], P(('dp', 'tp')), may hold values from -5 to 5
- cache_values: bfloat16 [256, 256, 8, 128], P(('dp', 'tp')), may hold values from -5 to 5
- lengths: int32 [256], P(('dp', 'tp')), may hold values from 2 to 256
Outputs:
- layer_out: bfloat16 [256, 8192], P(('dp', 'tp'))
The draws below stay inside these ranges and needn't reach their ends.
All inputs are finite; a program needn't handle non-finite values.
Results may differ from the reference program's by a relative error of at most 0.015.
Values may be sent and summed in bfloat16 or wider, within the bound.
No kernel may reach another device: no remote copies, remote signals or barrier semaphores. Data moves between devices by JAX's collectives and lax.ppermute only.
A program may use at most 256 MiB of HBM per device.

```python
import jax
import jax.numpy as jnp
from jax import lax

D = 8192
FF = 16384
HEADS = 64
KV_HEADS = 8
HEAD = 128
CACHE = 256
ROWS = 256


def shared_keys(key):
    raw = jax.random.normal(jax.random.fold_in(key, 11), (ROWS, CACHE, KV_HEADS, HEAD), jnp.float32)
    return jnp.clip(raw, -4.9, 4.9)


def draw_cache_keys(key, part):
    keys_all = shared_keys(key)
    return keys_all.astype(jnp.bfloat16)


def draw_queries(key, part):
    raw = jax.random.normal(jax.random.fold_in(key, 23), (ROWS, HEADS, HEAD), jnp.float32)
    values_out = jnp.clip(raw, -5.0, 5.0)
    return values_out.astype(jnp.bfloat16)


def touch_ends(drawn, rng, low, largest):
    place = [jax.random.randint(jax.random.fold_in(rng, axis), (), 0, length) for axis, length in enumerate(drawn.shape)]
    main_axis = drawn.shape.index(max(drawn.shape))
    neighbour = place[:main_axis] + [(place[main_axis] + 1) % drawn.shape[main_axis]] + place[main_axis + 1:]
    return drawn.at[tuple(place)].set(low).at[tuple(neighbour)].set(largest)


def block_levels(stream_key, dims, pieces, least, largest):
    loudness = 1.0
    for dim, blocks in pieces:
        draws = jax.random.uniform(jax.random.fold_in(jax.random.fold_in(stream_key, 6), dim), (blocks,), jnp.float32, least / len(pieces), largest / len(pieces))
        loudness = loudness * jnp.repeat(jnp.exp(draws), dims[dim] // blocks).reshape((-1,) + (1,) * (len(dims) - 1 - dim))
    return loudness


def centred(key, shape, deviation, reach, pieces=(), kind=jnp.bfloat16):
    array = deviation * jax.random.normal(key, shape, jnp.float32)
    if pieces:
        array = array * block_levels(key, shape, pieces, -0.22, 0.18)
    return jnp.clip(array, -reach, reach).astype(kind)


def setup_inputs(seed: int = 0) -> dict:
    seeds = jax.random.split(jax.random.key(seed), 13)
    gate_master = centred(seeds[0], (D, FF), D ** -0.5, 0.0625, ((0, 32),), jnp.float32)
    up_master = centred(seeds[1], (D, FF), D ** -0.5, 0.0625, ((0, 32),), jnp.float32)
    down_master = centred(seeds[2], (FF, D), FF ** -0.5, 0.046875, ((1, 32),), jnp.float32)
    out_proj = centred(seeds[3], (D, D), D ** -0.5, 0.0625, ((1, 8),))
    norm_gain = jnp.clip(1.0 + 0.18 * jax.random.normal(seeds[4], (D,), jnp.float32), 0.1, 1.9)
    residual_in = centred(seeds[5], (ROWS, D), 1.0, 6.0, ((0, 4), (1, 8)))
    queries = draw_queries(jax.random.fold_in(seeds[12], 71), 0)
    new_keys = centred(seeds[7], (ROWS, KV_HEADS, HEAD), 1.0, 5.0, ((0, 32),))
    new_values = centred(seeds[8], (ROWS, KV_HEADS, HEAD), 1.0, 5.0, ((0, 32),))
    cache_keys = draw_cache_keys(jax.random.fold_in(seeds[12], 71), 0)
    cache_values = centred(seeds[10], (ROWS, CACHE, KV_HEADS, HEAD), 1.0, 5.0, ((0, 32),))
    lengths = touch_ends(jax.random.randint(seeds[11], (ROWS,), 2, CACHE + 1), jax.random.fold_in(seeds[11], 1), 2, CACHE).astype(jnp.int32)
    return {"gate_master": gate_master, "up_master": up_master, "down_master": down_master, "out_proj": out_proj, "norm_gain": norm_gain, "residual_in": residual_in, "queries": queries, "new_keys": new_keys, "new_values": new_values, "cache_keys": cache_keys, "cache_values": cache_values, "lengths": lengths}


epsilon = 1e-06

def reference(gate_master, up_master, down_master, out_proj, norm_gain, residual_in, queries, new_keys, new_values, cache_keys, cache_values, lengths):
    row_count = queries.shape[0]
    group_size = HEADS // KV_HEADS
    factor = HEAD ** (-0.5)
    query_grid = queries.astype(jnp.float32).reshape(row_count, KV_HEADS, group_size, HEAD)
    scores = jnp.einsum('rkge,rlke->rkgl', query_grid, cache_keys.astype(jnp.float32)) * factor
    live_mask = (jnp.arange(CACHE, dtype=jnp.int32)[None, :] < lengths[:, None])[:, None, None, :]
    scores = jnp.where(live_mask, scores, -jnp.inf)
    score_new = jnp.einsum('rkge,rke->rkg', query_grid, new_keys.astype(jnp.float32)) * factor
    row_max = jnp.maximum(lax.optimization_barrier(jnp.max(scores, axis=-1)), score_new)
    powers = jnp.exp(scores - row_max[..., None])
    power_new = jnp.exp(score_new - row_max)
    summed = lax.optimization_barrier(jnp.sum(powers, axis=-1)) + power_new
    weights = (powers / summed[..., None]).astype(jnp.bfloat16)
    weight_new = (power_new / summed).astype(jnp.bfloat16)
    attended = jnp.einsum('rkgl,rlke->rkge', weights.astype(jnp.float32), cache_values.astype(jnp.float32))
    attended = attended + weight_new.astype(jnp.float32)[..., None] * new_values.astype(jnp.float32)[:, :, None, :]
    attended = attended.reshape(row_count, D).astype(jnp.bfloat16)
    projected = jnp.dot(attended, out_proj, preferred_element_type=jnp.float32)
    residual_mid = (residual_in.astype(jnp.float32) + projected).astype(jnp.bfloat16)
    middle = residual_mid.astype(jnp.float32)
    normed = (middle * lax.rsqrt(lax.optimization_barrier(jnp.mean(middle * middle, axis=-1, keepdims=True)) + epsilon) * norm_gain).astype(jnp.bfloat16)
    gate_value = jnp.dot(normed, gate_master.astype(jnp.bfloat16), preferred_element_type=jnp.float32)
    up_value = jnp.dot(normed, up_master.astype(jnp.bfloat16), preferred_element_type=jnp.float32)
    hidden = (jax.nn.silu(gate_value) * up_value).astype(jnp.bfloat16)
    mlp_rows = jnp.dot(hidden, down_master.astype(jnp.bfloat16), preferred_element_type=jnp.float32)
    return (middle + mlp_rows).astype(jnp.bfloat16)
```

```python
import math

import jax
import jax.numpy as jnp
from jax import lax
from jax.experimental import pallas as pl
from jax.experimental.pallas import tpu as pltpu
from jax.sharding import Mesh, PartitionSpec as P


CHUNKS = 4
epsilon = 1e-06
f32, bf16 = jnp.float32, jnp.bfloat16


def attend(queries, new_keys, new_values, cache_keys, cache_values, lengths):
    row_count, heads, head = queries.shape
    cache, kv_heads = cache_keys.shape[1], cache_keys.shape[2]
    factor = head ** (-0.5)
    query_grid = queries.reshape(row_count, kv_heads, heads // kv_heads, head)
    scores = (
        jnp.einsum("rkge,rlke->rkgl", query_grid, cache_keys, preferred_element_type=f32)
        * factor
    )
    slots = lax.broadcasted_iota(jnp.int32, (row_count, cache), 1)
    live_mask = (slots < lengths[:, None])[:, None, None, :]
    scores = jnp.where(live_mask, scores, -jnp.inf)
    score_new = (
        jnp.einsum("rkge,rke->rkg", query_grid, new_keys, preferred_element_type=f32) * factor
    )
    row_max = jnp.maximum(jnp.max(scores, axis=-1), score_new)
    powers = jnp.exp(scores - row_max[..., None])
    power_new = jnp.exp(score_new - row_max)
    summed = jnp.sum(powers, axis=-1) + power_new
    weights = (powers / summed[..., None]).astype(bf16)
    weight_new = (power_new / summed).astype(bf16)
    attended = jnp.einsum("rkgl,rlke->rkge", weights, cache_values, preferred_element_type=f32)
    attended = (
        attended + weight_new.astype(f32)[..., None] * new_values.astype(f32)[:, :, None, :]
    )
    return attended.reshape(row_count, heads * head).astype(bf16)


def factor_axis(points):
    dims, stride = [], 1
    while stride < len(points):
        moved = [k for k in range(4) if points[stride][k] != points[0][k]]
        (which,) = moved
        size = 2
        while size * stride < len(points) and all(
            points[size * stride][k] == points[0][k] for k in range(4) if k != which
        ):
            size += 1
        dims.append((which, size))
        stride *= size
    return dims[::-1]


def shift(value, axis, size, by):
    return lax.ppermute(value, axis, [(i, (i + by) % size) for i in range(size)])


def unroll_rows(value, names, sizes):
    rows = value.shape[0] // math.prod(sizes)
    value = value.reshape(*sizes, rows, *value.shape[1:])
    for at, (name, size) in enumerate(zip(names, sizes)):
        back = lax.rem(size - lax.axis_index(name), size)
        twice = jnp.concatenate([value, value], axis=at)
        value = lax.dynamic_slice_in_dim(twice, back, size, at)
    return value.reshape(-1, *value.shape[len(sizes) + 1 :])


def block_order(order, sizes):
    index = jnp.zeros((), jnp.int32)
    for name in order:
        size = sizes[name]
        here = lax.rem(lax.axis_index(name) + jnp.arange(size, dtype=jnp.int32), size)
        index = index[..., None] * size + here
    return index.reshape(-1)


def cast_columns(first, second, which, index, width):
    rows = first.shape[0]
    chunks, count = index.shape
    span = count * width
    if width % 128 or rows % 16:
        places = ((which * chunks + jnp.arange(chunks))[:, None] * count + index).reshape(-1)
        picked = [
            jnp.take(m.reshape(rows, -1, width), places, axis=1).reshape(rows, chunks * span)
            for m in (first, second)
        ]
        return jnp.stack(picked).astype(bf16)

    def body(which_ref, index_ref, first_ref, second_ref, out_ref):
        chunk = pl.program_id(0)
        for b in range(count):
            source = pl.ds(pl.multiple_of(index_ref[chunk, b] * width, width), width)
            out_ref[0, :, b * width : (b + 1) * width] = first_ref[:, source].astype(bf16)
            out_ref[1, :, b * width : (b + 1) * width] = second_ref[:, source].astype(bf16)

    source = pl.BlockSpec((rows, span), lambda k, w, i: (0, w[0] * chunks + k))
    return pl.pallas_call(
        body,
        out_shape=jax.ShapeDtypeStruct((2, rows, chunks * span), bf16),
        grid_spec=pltpu.PrefetchScalarGridSpec(
            num_scalar_prefetch=2,
            grid=(chunks,),
            in_specs=[source, source],
            out_specs=pl.BlockSpec((2, rows, span), lambda k, w, i: (0, 0, k)),
        ),
        cost_estimate=pl.CostEstimate(
            flops=rows * chunks * span * 512,
            bytes_accessed=12 * rows * chunks * span,
            transcendentals=0,
        ),
        compiler_params=pltpu.CompilerParams(vmem_limit_bytes=32 * 1024 * 1024),
        name="cast_columns",
    )(which.reshape(1), index, first, second)


def cast_rows(matrix, which, index, height):
    columns = matrix.shape[1]
    chunks, count = index.shape
    span = count * height
    if height % 16 or columns % 128:
        places = ((which * chunks + jnp.arange(chunks))[:, None] * count + index).reshape(-1)
        picked = jnp.take(matrix.reshape(-1, height, columns), places, axis=0)
        return picked.reshape(chunks * span, columns).astype(bf16)

    def body(which_ref, index_ref, in_ref, out_ref):
        chunk = pl.program_id(0)
        for b in range(count):
            source = pl.ds(pl.multiple_of(index_ref[chunk, b] * height, height), height)
            out_ref[b * height : (b + 1) * height, :] = in_ref[source, :].astype(bf16)

    return pl.pallas_call(
        body,
        out_shape=jax.ShapeDtypeStruct((chunks * span, columns), bf16),
        grid_spec=pltpu.PrefetchScalarGridSpec(
            num_scalar_prefetch=2,
            grid=(chunks,),
            in_specs=[pl.BlockSpec((span, columns), lambda k, w, i: (w[0] * chunks + k, 0))],
            out_specs=pl.BlockSpec((span, columns), lambda k, w, i: (k, 0)),
        ),
        cost_estimate=pl.CostEstimate(
            flops=columns * chunks * span * 256,
            bytes_accessed=6 * columns * chunks * span,
            transcendentals=0,
        ),
        compiler_params=pltpu.CompilerParams(vmem_limit_bytes=32 * 1024 * 1024),
        name="cast_rows",
    )(which.reshape(1), index, matrix)


def partial_products(inputs, weights, start, count):
    rows = inputs[0].shape[0]
    width = math.gcd(count, 512)
    depth = sum(x.shape[1] for x in inputs)

    def body(*refs):
        xs, ws, out_ref = refs[: len(inputs)], refs[len(inputs) : -1], refs[-1]
        for which in range(2):
            total = sum(
                jnp.dot(x[...], w[which], preferred_element_type=f32) for x, w in zip(xs, ws)
            )
            out_ref[which] = total.astype(bf16)

    if start % width or width % 128:
        total = sum(
            jnp.einsum("rk,gkc->grc", x, w[:, :, start : start + count], preferred_element_type=f32)
            for x, w in zip(inputs, weights)
        )
        return total.astype(bf16)
    return pl.pallas_call(
        body,
        out_shape=jax.ShapeDtypeStruct((2, rows, count), bf16),
        grid=(count // width,),
        in_specs=[pl.BlockSpec(x.shape, lambda k: (0, 0)) for x in inputs]
        + [
            pl.BlockSpec((2, w.shape[1], width), lambda k: (0, 0, k + start // width))
            for w in weights
        ],
        out_specs=pl.BlockSpec((2, rows, width), lambda k: (0, 0, k)),
        cost_estimate=pl.CostEstimate(
            flops=4 * rows * depth * count,
            bytes_accessed=4 * (depth + rows) * count,
            transcendentals=0,
        ),
        compiler_params=pltpu.CompilerParams(vmem_limit_bytes=48 * 1024 * 1024),
        name="partial_products",
    )(*inputs, *weights)


def solution(mesh):
    devices = mesh.devices
    dp_axis, tp_axis = mesh.axis_names
    place = lambda d: (*d.coords, d.core_on_chip)
    dp_dims = factor_axis([place(d) for d in devices[:, 0]])
    tp_dims = factor_axis([place(d) for d in devices[0, :]])
    dp_names = tuple(("core" if w == 3 else f"dp{k}") for k, (w, _) in enumerate(dp_dims))
    tp_names = tuple(f"tp{k}" for k in range(len(tp_dims)))
    names = dp_names + tp_names
    sizes = dict(zip(names, [n for _, n in dp_dims + tp_dims]))
    grid = Mesh(devices.reshape([sizes[n] for n in names]), names)
    dp_size, tp_size = devices.shape
    cores = sizes["core"]
    chip_names = sorted((n for n in names if n != "core"), key=lambda n: sizes[n])
    chips = math.prod(sizes[n] for n in chip_names)
    tp_order = sorted(tp_names, key=lambda n: -sizes[n])

    def gather_rows(value):
        pieces = [value]
        for name in tp_order:
            size = sizes[name]
            pieces = [
                p if s == 0 else shift(p, name, size, -s) for s in range(size) for p in pieces
            ]
        return jnp.concatenate(pieces, axis=0), tuple(reversed(tp_order))

    def per_device(
        gate_master,
        up_master,
        down_master,
        out_proj,
        norm_gain,
        residual_in,
        queries,
        new_keys,
        new_values,
        cache_keys,
        cache_values,
        lengths,
    ):
        rows_dev = queries.shape[0]
        depth, hidden_all = gate_master.shape
        width_model = out_proj.shape[0]
        rows_all = rows_dev * dp_size * tp_size
        core = lax.axis_index("core")
        me = lax.axis_index(names)

        half = hidden_all // cores
        part = half // CHUNKS
        width = part // chips
        orders = []
        for k in range(CHUNKS):
            order = list(chip_names)
            if k % 2:
                order[0], order[1] = order[1], order[0]
            orders.append(order)
        places = jnp.stack([block_order(orders[k], sizes) for k in range(CHUNKS)])

        attended = attend(queries, new_keys, new_values, cache_keys, cache_values, lengths)
        rows_near, near_order = gather_rows(attended)

        away = lax.rem(core + 1, cores)
        sent_gu = cast_columns(gate_master, up_master, away, places, width)
        held_gu = cast_columns(gate_master, up_master, core, places, width)
        got_gu = shift(sent_gu, "core", cores, 1)
        sent_d = cast_rows(down_master, away, places, width)
        held_d = cast_rows(down_master, core, places, width)
        got_d = shift(sent_d, "core", cores, 1)

        projected = jnp.dot(rows_near, out_proj, preferred_element_type=f32)
        near_sizes = [sizes[n] for n in near_order]
        projected = unroll_rows(projected, near_order, near_sizes)
        projected = projected.reshape(*near_sizes, rows_dev, -1)
        projected = projected.transpose(
            *[near_order.index(n) for n in tp_names], len(tp_names), len(tp_names) + 1
        ).reshape(rows_dev * tp_size, -1)
        mid = (residual_in.astype(f32) + projected).astype(bf16)
        wide = mid.astype(f32)
        square = jnp.sum(wide * wide, axis=-1, keepdims=True)
        s0 = square.astype(bf16)
        s1 = (square - s0.astype(f32)).astype(bf16)
        s2 = (square - s0.astype(f32) - s1.astype(f32)).astype(bf16)
        extra = jnp.concatenate(
            [s0, s1, s2, jnp.zeros((mid.shape[0], 125), bf16)], axis=1
        )
        columns = mid.reshape(mid.shape[0], dp_size, depth)
        payload = jnp.concatenate(
            [columns, jnp.broadcast_to(extra[:, None, :], (mid.shape[0], dp_size, 128))], axis=2
        )
        payload = payload.transpose(1, 0, 2)
        payload = lax.all_to_all(payload, dp_names, 0, 0, tiled=True)
        payload = payload.reshape(rows_all, depth + 128)
        total = payload[:, depth : depth + 3].astype(f32)
        total = jnp.sum(total, axis=-1).reshape(1, rows_all)

        pairs = [
            (q * tp_size + j, j * dp_size + q) for q in range(dp_size) for j in range(tp_size)
        ]
        middle = lax.ppermute(payload[:, :depth], names, pairs)
        for name in tp_order[::-1]:
            total = sum(
                (shift(total, name, sizes[name], s) for s in range(1, sizes[name])), total
            )
        scale = lax.rsqrt(total / width_model + epsilon).reshape(rows_all, 1)

        gain = lax.dynamic_slice_in_dim(norm_gain, me * depth, depth)
        near = (middle.astype(f32) * gain).astype(bf16)
        far = shift(near, "core", cores, 1)
        inputs, weights = [near, far], [held_gu, got_gu]

        def scatter_chunk(k):
            order = orders[k]
            start, count = k * part, part
            first = sizes[order[0]]
            piece = count // first
            sent = [
                partial_products(inputs, weights, start + s * piece, piece)
                for s in range(1, first)
            ]
            arrived = [shift(v, order[0], first, s + 1) for s, v in enumerate(sent)]
            own = partial_products(inputs, weights, start, piece)
            for name in order[1:]:
                size = sizes[name]
                piece = piece // size
                cut = lambda s: sum(
                    (v[:, :, s * piece : (s + 1) * piece].astype(f32) for v in [own, *arrived])
                )
                pieces = [cut(s).astype(bf16) for s in range(size)]
                arrived = [shift(pieces[s], name, size, s) for s in range(1, size)]
                own = pieces[0]
            value = sum(v.astype(f32) for v in [own, *arrived]) * scale
            return (jax.nn.silu(value[0]) * value[1]).astype(bf16)

        def gather_chunk(hidden, k):
            for name in orders[k][::-1]:
                size = sizes[name]
                blocks = [hidden] + [shift(hidden, name, size, -s) for s in range(1, size)]
                hidden = jnp.concatenate(blocks, axis=1)
            return hidden

        hidden = [gather_chunk(scatter_chunk(k), k) for k in range(CHUNKS)]
        near_out = far_out = 0.0
        for k in range(CHUNKS):
            rows = slice(k * part, (k + 1) * part)
            near_out += jnp.dot(hidden[k], held_d[rows], preferred_element_type=f32)
            far_out += jnp.dot(hidden[k], got_d[rows], preferred_element_type=f32)
        own_out = near_out + shift(far_out.astype(bf16), "core", cores, 1).astype(f32)
        own_out = (own_out + middle.astype(f32)).astype(bf16)
        rows_out = lax.all_to_all(own_out, names, 0, 1, tiled=True)
        return rows_out

    placed = (
        P(names, None),
        P(names, None),
        P(None, names),
        P(None, tp_names),
        P(),
        P(dp_names, tp_names),
        P(names, None, None),
        P(names, None, None),
        P(names, None, None),
        P(names, None, None, None),
        P(names, None, None, None),
        P(names),
    )
    return jax.shard_map(
        per_device, mesh=grid, in_specs=placed, out_specs=P(names, None), check_vma=False
    )
```
